32 devices in a mesh: outer: 4 (over y, x), inner: 8 (over z, core).
Axes of the slice: x: 2, y: 2, z: 4, core: 2. Of those that a mesh axis runs over, the one named last changes fastest.
Arguments:
- query_states: bfloat16 [4096, 2048], P(('outer', 'inner')), may hold values from -400 to 400
- key_states: bfloat16 [4096, 2048], P(('outer', 'inner')), may hold values from -13 to 13
- value_states: bfloat16 [4096, 2048], P(('outer', 'inner')), may hold values from -27 to 27
Outputs:
- attention_out: bfloat16 [4096, 2048], P(('outer', 'inner'))
The draws below stay inside these ranges and needn't reach their ends.
All inputs are finite; a program needn't handle non-finite values.
Results may differ from the reference program's by a relative error of at most 0.0038.
Values may be sent and summed in bfloat16 or wider, within the bound.
No kernel may reach another device: no remote copies, remote signals or barrier semaphores. Data moves between devices by JAX's collectives and lax.ppermute only.
A program may use at most 64 MiB of HBM per device.

```python
import math
import jax
import jax.numpy as jnp
from jax import lax

HEADS = 16
HEAD_DIM = 128
LEAF = 128
WIDTH = 2048
SEQ = 4096
N_INNER = 8


def layered(seed_key, columns):
    layers_count = min(SEQ.bit_length() - 1, 16) + 1
    running = jax.random.truncated_normal(jax.random.fold_in(seed_key, layers_count - 1), -3.0, 3.0, (SEQ >> layers_count - 1, columns), jnp.float32)
    for layer_index in range(layers_count - 2, -1, -1):
        fresh = jax.random.truncated_normal(jax.random.fold_in(seed_key, layer_index), -3.0, 3.0, (SEQ >> layer_index, columns), jnp.float32)
        running = jnp.repeat(running, 2, axis=0) + fresh
    return running / math.sqrt(layers_count)


def draw_query_states(key, part):
    drawn = 1.25 * layered(jax.random.fold_in(key, 1), WIDTH)
    return drawn.astype(jnp.bfloat16)


def draw_key_states(key, part):
    base_draw = layered(jax.random.fold_in(key, 2), WIDTH)
    return base_draw.astype(jnp.bfloat16)


def draw_value_states(key, part):
    base_draw = 2.0 * layered(jax.random.fold_in(key, 3), WIDTH)
    return base_draw.astype(jnp.bfloat16)


def setup_inputs(seed: int = 0) -> dict:
    streams_of = jax.random.split(jax.random.key(seed), 4)
    return {
        "query_states": draw_query_states(jax.random.fold_in(streams_of[3], 71), 0),
        "key_states": draw_key_states(jax.random.fold_in(streams_of[3], 71), 0),
        "value_states": draw_value_states(jax.random.fold_in(streams_of[3], 71), 0),
    }


def halve_rows(array):
    paired = array.astype(jnp.float32).reshape(array.shape[0] // 2, 2, array.shape[1])
    return lax.optimization_barrier(((paired[:, 0] + paired[:, 1]) * 0.5).astype(jnp.bfloat16))

def level_terms(query_rows, key_rows, value_rows):
    shaped_q = query_rows.astype(jnp.float32).reshape(query_rows.shape[0], HEADS, HEAD_DIM)
    shaped_k = key_rows.astype(jnp.float32).reshape(key_rows.shape[0], HEADS, HEAD_DIM)
    shaped_v = value_rows.astype(jnp.float32).reshape(value_rows.shape[0], HEADS, HEAD_DIM)
    scores = jnp.einsum('rhe,che->hrc', shaped_q, shaped_k, precision=lax.Precision.HIGHEST) / math.sqrt(HEAD_DIM)
    peak_scores = lax.optimization_barrier(jnp.max(scores, axis=2))
    weights = jnp.exp(scores - peak_scores[:, :, None])
    totals = lax.optimization_barrier(jnp.sum(weights, axis=2))
    rounded = lax.optimization_barrier(weights.astype(jnp.bfloat16)).astype(jnp.float32)
    weighted = jnp.einsum('hrc,che->hre', rounded, shaped_v, precision=lax.Precision.HIGHEST)
    return (peak_scores, totals, weighted)

def spread_rows(terms, factor):
    return tuple((jnp.repeat(member, factor, axis=1) for member in terms))

def combine(level_parts):
    highest = level_parts[0][0]
    for member in level_parts[1:]:
        highest = jnp.maximum(highest, member[0])
    numerator = jnp.zeros(level_parts[0][2].shape, jnp.float32)
    denominator = jnp.zeros(level_parts[0][1].shape, jnp.float32)
    for member in level_parts:
        factor = jnp.exp(member[0] - highest)
        numerator = numerator + factor[:, :, None] * member[2]
        denominator = denominator + factor * member[1]
    result = numerator / denominator[:, :, None]
    return jnp.transpose(result, (1, 0, 2)).reshape(result.shape[1], HEADS * HEAD_DIM).astype(jnp.bfloat16)

def reference(query_states, key_states, value_states):
    top_level = (2 * N_INNER).bit_length() - 1
    block_count = SEQ // LEAF
    pooled_keys = [key_states]
    pooled_values = [value_states]
    for level_index in range(top_level):
        pooled_keys.append(halve_rows(pooled_keys[-1]))
        pooled_values.append(halve_rows(pooled_values[-1]))

    def one_block(block_index):
        row_start = (block_index * LEAF).astype(jnp.int32)
        query_rows = lax.dynamic_slice_in_dim(query_states, row_start, LEAF, 0)
        pair_start = (block_index // 2 * (2 * LEAF)).astype(jnp.int32)
        near_keys = lax.dynamic_slice_in_dim(key_states, pair_start, 2 * LEAF, 0)
        near_values = lax.dynamic_slice_in_dim(value_states, pair_start, 2 * LEAF, 0)
        level_parts = [level_terms(query_rows, near_keys, near_values)]
        coarse = query_rows
        for level_index in range(1, top_level + 1):
            coarse = halve_rows(coarse)
            partner = ((jnp.right_shift(block_index, level_index) ^ 1) * LEAF).astype(jnp.int32)
            far_keys = lax.dynamic_slice_in_dim(pooled_keys[level_index], partner, LEAF, 0)
            far_values = lax.dynamic_slice_in_dim(pooled_values[level_index], partner, LEAF, 0)
            terms = level_terms(coarse, far_keys, far_values)
            level_parts.append(spread_rows(terms, 2 ** level_index))
        return combine(level_parts)
    outputs = lax.map(one_block, jnp.arange(block_count, dtype=jnp.int32))
    return outputs.reshape(SEQ, HEADS * HEAD_DIM)
```

```python
import functools
import math

import jax
import jax.numpy as jnp
from jax import lax
from jax.experimental import pallas as pl
from jax.experimental.pallas import tpu as pltpu
from jax.sharding import PartitionSpec as P

HEAD_DIM = 128
LANES = 128
PIECES = 3
F32 = jnp.float32
BF16 = jnp.bfloat16


def dot(a, b):
    return lax.dot_general(a, b, (((1,), (0,)), ((), ())), preferred_element_type=F32)


def dot_t(a, b):
    return lax.dot_general(a, b, (((1,), (1,)), ((), ())), preferred_element_type=F32)


def halving(rows):
    row = lax.broadcasted_iota(jnp.int32, (rows // 2, rows), 0)
    column = lax.broadcasted_iota(jnp.int32, (rows // 2, rows), 1)
    return jnp.where(jnp.right_shift(column, 1) == row, 0.5, 0.0).astype(BF16)


def averaging(rows, distance):
    row = lax.broadcasted_iota(jnp.int32, (rows, rows), 0)
    column = lax.broadcasted_iota(jnp.int32, (rows, rows), 1)
    return jnp.where((column == row) | (column == row ^ distance), 0.5, 0.0).astype(BF16)


def halve(x):
    return dot(halving(x.shape[0]), x).astype(BF16)


def kernel_call(body, outs, scratch=(), name=None):
    def call(*operands):
        return pl.pallas_call(
            body,
            out_shape=[jax.ShapeDtypeStruct(shape, dtype) for shape, dtype in outs],
            in_specs=[pl.BlockSpec(memory_space=pltpu.VMEM)] * len(operands),
            out_specs=[pl.BlockSpec(memory_space=pltpu.VMEM)] * len(outs),
            scratch_shapes=list(scratch),
            name=name,
        )(*operands)

    return call


def pool_body(near, q_ref, k_ref, v_ref, *outs):
    for part, ref in enumerate((k_ref, v_ref)):
        rows = ref[...]
        for level in range(near):
            rows = halve(rows)
            outs[level][part] = rows
    rows = q_ref[...]
    for level in range(near + 2):
        rows = halve(rows)
        if level >= near:
            outs[level][...] = rows


def visit_body(near, scale, own_ref, other_ref_k, other_ref_v, *refs):
    counts = [2 << level for level in range(near)]
    far = refs[: sum(counts)]
    q_one, q_two, q_three = refs[sum(counts) : sum(counts) + 3]
    outs = refs[sum(counts) + 3 : sum(counts) + 6]
    joined, queries = refs[-2:]
    leaf = other_ref_k.shape[0]
    half = leaf // 2
    joined[0, :half] = own_ref[0]
    joined[1, :half] = own_ref[1]
    joined[0, half:leaf] = halve(other_ref_k[...])
    joined[1, half:leaf] = halve(other_ref_v[...])
    start = 0
    for level in range(near):
        size = leaf >> (level + 1)
        for place in range(counts[level]):
            at = leaf + place * size
            for part in range(2):
                joined[part, at : at + size] = far[start + place][part]
        start += counts[level]
        pooled = [halve(joined[part]) for part in range(2)]
        for part in range(2):
            joined[part, :leaf] = pooled[part]
    for part in range(2):
        joined[part, leaf : leaf + half] = halve(joined[part, :leaf])
    keys = leaf + half

    first, second = q_one.shape[0], q_two.shape[0]
    total = first + 2 * second
    queries[:first] = q_one[...]
    queries[first : first + second] = q_two[...]
    queries[first + second : total] = q_three[...]
    row = lax.broadcasted_iota(jnp.int32, (total, keys), 0)
    column = lax.broadcasted_iota(jnp.int32, (total, keys), 1)
    allowed = (row < first) == (column < leaf)
    lane = lax.broadcasted_iota(jnp.int32, (total, LANES), 1)
    width = q_one.shape[1]
    heads = width // HEAD_DIM
    stats = jnp.zeros((total, LANES), F32)
    for head in range(heads):
        at = slice(head * HEAD_DIM, (head + 1) * HEAD_DIM)
        scores = dot_t(queries[:, at], joined[0, :keys, at])
        scores = jnp.where(allowed, scores, -jnp.inf)
        peak = jnp.max(scores, axis=1, keepdims=True)
        weights = jnp.exp2((scores - peak) * scale)
        den = jnp.sum(weights, axis=1, keepdims=True)
        num = dot(weights.astype(BF16), joined[1, :keys, at]).astype(BF16)
        outs[0][:, at] = num[:first]
        outs[1][:, at] = num[first : first + second]
        outs[2][:, at] = num[first + second :]
        stats = jnp.where(lane == head, peak, stats)
        stats = jnp.where(lane == heads + head, den, stats)
    for piece in range(PIECES):
        part = stats.astype(BF16)
        stats = stats - part.astype(F32)
        at = slice(width + piece * LANES, width + (piece + 1) * LANES)
        outs[0][:, at] = part[:first]
        outs[1][:, at] = part[first : first + second]
        outs[2][:, at] = part[first + second :]


def local_body(near, scale, q_ref, k_ref, v_ref, other_ref_k, other_ref_v, *refs):
    counts = [2 << level for level in range(near)]
    far = refs[: sum(counts)]
    num_ref, stat_ref = refs[sum(counts) : sum(counts) + 2]
    joined, queries = refs[-2:]
    leaf, width = q_ref.shape
    heads = width // HEAD_DIM
    start = 0
    rows = q_ref[...]
    for level in range(near):
        size = leaf >> (level + 1)
        for place in range(counts[level]):
            at = place * size
            for part in range(2):
                joined[level, part, at : at + size] = far[start + place][part]
        start += counts[level]
        rows = dot(averaging(leaf, 1 << level), rows).astype(BF16)
        queries[level] = rows
    lane = lax.broadcasted_iota(jnp.int32, (leaf, LANES), 1)
    stats = jnp.zeros((leaf, LANES), F32)
    for head in range(heads):
        at = slice(head * HEAD_DIM, (head + 1) * HEAD_DIM)
        scores = [dot_t(q_ref[:, at], k_ref[:, at]), dot_t(q_ref[:, at], other_ref_k[:, at])]
        values = [v_ref[:, at], other_ref_v[:, at]]
        for level in range(near):
            scores.append(dot_t(queries[level, :, at], joined[level, 0, :, at]))
            values.append(joined[level, 1, :, at])
        top = functools.reduce(jnp.maximum, scores)
        peak = jnp.max(top, axis=1, keepdims=True)
        weights = [jnp.exp2((member - peak) * scale) for member in scores]
        den = jnp.sum(functools.reduce(jnp.add, weights), axis=1, keepdims=True)
        num = functools.reduce(
            jnp.add, [dot(member.astype(BF16), value) for member, value in zip(weights, values)]
        )
        num_ref[:, at] = num
        stats = jnp.where(lane == head, peak, stats)
        stats = jnp.where(lane == heads + head, den, stats)
    stat_ref[...] = stats


def merge_body(scale, num_ref, stat_ref, *refs):
    results, out_ref = refs[:-1], refs[-1]
    leaf, width = num_ref.shape
    heads = width // HEAD_DIM
    spreads, stats = [], [stat_ref[...]]
    for ref in results:
        count = ref.shape[0]
        row = lax.broadcasted_iota(jnp.int32, (leaf, count), 0)
        column = lax.broadcasted_iota(jnp.int32, (leaf, count), 1)
        shift = (leaf // count).bit_length() - 1
        spread = (jnp.right_shift(row, shift) == column).astype(F32).astype(BF16)
        spreads.append(spread)
        stat = 0.0
        for piece in range(PIECES):
            at = slice(width + piece * LANES, width + (piece + 1) * LANES)
            stat = stat + dot(spread, ref[:, at])
        stats.append(stat)
    top = functools.reduce(jnp.maximum, stats)
    factors = [jnp.exp2((stat - top) * scale) for stat in stats]
    lane = lax.broadcasted_iota(jnp.int32, (leaf, LANES), 1)
    total = 0.0
    for factor, stat in zip(factors, stats):
        total = total + jnp.where(lane < heads, factor, 0.0) * pltpu.roll(stat, LANES - heads, 1)
    inverse = 1.0 / jnp.where(lane < heads, total, 1.0)
    factors = [factor * inverse for factor in factors]
    for head in range(heads):
        at = slice(head * HEAD_DIM, (head + 1) * HEAD_DIM)
        value = factors[0][:, head : head + 1] * num_ref[:, at]
        for factor, spread, ref in zip(factors[1:], spreads, results):
            value = value + factor[:, head : head + 1] * dot(spread, ref[:, at])
        out_ref[:, at] = value.astype(BF16)


def body(query_states, key_states, value_states):
    inner = lax.axis_size("inner")
    outer = lax.axis_size("outer")
    near = inner.bit_length() - 2
    leaf, width = query_states.shape
    scale = math.log2(math.e) / math.sqrt(HEAD_DIM)

    def within(block, mask):
        return lax.ppermute(block, "inner", [(place, place ^ mask) for place in range(inner)])

    def across(block, mask):
        return lax.ppermute(block, "outer", [(place, place ^ mask) for place in range(outer)])

    pooled_shapes = [((2, leaf >> level, width), BF16) for level in range(1, near + 1)]
    query_shapes = [((leaf >> level, width), BF16) for level in (near + 1, near + 2)]
    pooled = kernel_call(
        functools.partial(pool_body, near), pooled_shapes + query_shapes, name="pool"
    )(query_states, key_states, value_states)
    other_k, other_v = within(key_states, 1), within(value_states, 1)
    far = []
    for level in reversed(range(near)):
        own = [within(pooled[level], 2 * place) for place in range(1 << level, 2 << level)]
        far.append(own)
    far = far[::-1]
    visitors = (
        across(pooled[near], 1),
        across(pooled[near + 1], 2),
        across(pooled[near + 1], 3),
    )
    far = [member for own in far for got in own for member in (got, within(got, 1))]
    extra = PIECES * LANES
    first, second = leaf >> near + 1, leaf >> near + 2
    results = kernel_call(
        functools.partial(visit_body, near, scale),
        [((rows, width + extra), BF16) for rows in (first, second, second)],
        scratch=(
            pltpu.VMEM((2, 2 * leaf, width), BF16),
            pltpu.VMEM((first + 2 * second, width), BF16),
        ),
        name="visit",
    )(pooled[0], other_k, other_v, *far, *visitors)
    results = [across(result, mask) for result, mask in zip(results, (1, 2, 3))]
    num, stats = kernel_call(
        functools.partial(local_body, near, scale),
        [((leaf, width), F32), ((leaf, LANES), F32)],
        scratch=(
            pltpu.VMEM((near, 2, leaf, width), BF16),
            pltpu.VMEM((near, leaf, width), BF16),
        ),
        name="local",
    )(query_states, key_states, value_states, other_k, other_v, *far)
    (out,) = kernel_call(
        functools.partial(merge_body, scale), [((leaf, width), BF16)], name="merge"
    )(num, stats, *results)
    return out


def solution(mesh):
    placed = P(("outer", "inner"), None)
    return jax.shard_map(
        body, mesh=mesh, in_specs=(placed,) * 3, out_specs=placed, check_vma=False
    )
```
